256 devices in a mesh: level: 4 (over y), blk: 64 (over x, z, core).
Axes of the slice: x: 4, y: 4, z: 8, core: 2. Of those that a mesh axis runs over, the one named last changes fastest.
Arguments:
- right_sides: float32 [4, 512, 16384], P('level', None, 'blk'), may hold values from -6 to 6
- leaf_gen: float32 [4, 16384, 256], P('level', 'blk'), may hold values from -1 to 1, as said below
- leaf_inverse: float32 [4, 8192, 128], P('level', 'blk'), may hold values from -0.5 to 0.5
- leaf_lower: float32 [4, 8192, 128], P('level', 'blk'), may hold values from -0.5 to 0.5
- node_gen: float32 [4, 64, 6, 256, 256], P('level', 'blk'), may hold values from -1 to 1, as said below
- node_inverse: float32 [4, 64, 6, 128, 128], P('level', 'blk'), may hold values from -1 to 1, as said below
- node_lower: float32 [4, 64, 6, 128, 128], P('level', 'blk'), may hold values from -1 to 1, as said below
- coupling: float32 [4, 128, 256], P('level'), may hold values from -0.5 to 0.5
- child_leaf: int32 [4], P('level'), may hold values from 0 to 63
Outputs:
- leaf_solution: float32 [4, 512, 8192], P('level', None, 'blk')
- node_solution: float32 [4, 64, 6, 512, 128], P('level', 'blk')
- root_skeleton: float32 [4, 512, 128], P('level')
The draws below stay inside these ranges and needn't reach their ends.
Inputs may be any that keep to these rules, and one draw needn't show every extreme that they name: `leaf_gen`: each leaf's 256 x 256 block is orthogonal. node_gen[p, i, h] is orthogonal and equal for all leaves i with the same i >> (h + 1). node_inverse[p, i, h] is equal for all leaves i with the same i >> (h + 1). node_lower[p, i, h] is equal for all leaves i with the same i >> (h + 1).
All inputs are finite; a program needn't handle non-finite values.
Results may differ from the reference program's by a relative error of at most 0.0003.
Values sent between devices are 32-bit elements; how exact they have to be, the bound alone decides.
A program may use at most 64 MiB of HBM per device.

```python
import jax
import jax.numpy as jnp
from jax import lax

LEAF = 256
R = 128
NRHS = 512
RED = 128
LEAVES = 64
LEVELS = 4
FRONT = 16384
HEIGHT = 6


def orthogonal_stack(key, array_shape):
    values = jax.random.normal(key, array_shape, jnp.float32)
    factor, upper_part = jnp.linalg.qr(values)
    return factor


def node_draw(key, row_count, col_count, draw_kind, spread_factor):
    layers = []
    for tier_index in range(HEIGHT):
        group_span = 2 ** (tier_index + 1)
        array_shape = (LEVELS, LEAVES // group_span, row_count, col_count)
        subkey = jax.random.fold_in(key, 17 + tier_index)
        if draw_kind == 0:
            values = orthogonal_stack(subkey, array_shape)
        else:
            values = jax.random.truncated_normal(subkey, -4.0, 4.0, array_shape, jnp.float32) * spread_factor
        layers.append(jnp.repeat(values, group_span, axis=1))
    return jnp.stack(layers, axis=2)


def draw_leaf_gen(key, part):
    values = orthogonal_stack(jax.random.fold_in(key, 3), (LEVELS, LEAVES, LEAF, LEAF))
    return values.reshape(LEVELS, LEAVES * LEAF, LEAF)


def draw_node_gen(key, part):
    return node_draw(jax.random.fold_in(key, 5), 2 * R, 2 * R, 0, 1.0)


def draw_node_inverse(key, part):
    return node_draw(jax.random.fold_in(key, 7), R, R, 1, R ** (-0.5))


def draw_node_lower(key, part):
    return node_draw(jax.random.fold_in(key, 11), R, R, 1, 0.5 * R ** (-0.5))


def plant(entries, rng, smallest, high):
    spot = [jax.random.randint(jax.random.fold_in(rng, axis), (), 0, length) for axis, length in enumerate(entries.shape)]
    main_axis = entries.shape.index(max(entries.shape))
    beside = spot[:main_axis] + [(spot[main_axis] + 1) % entries.shape[main_axis]] + spot[main_axis + 1:]
    return entries.at[tuple(spot)].set(smallest).at[tuple(beside)].set(high)


def block_levels(own_key, shape, cuts, least, high):
    loudness, own = 1.0, jax.random.fold_in(own_key, 6)
    for position, shards_of in cuts:
        steps = jnp.exp(jax.random.uniform(jax.random.fold_in(own, position), (shards_of,), jnp.float32, least / len(cuts), high / len(cuts)))
        loudness = loudness * jnp.repeat(steps, shape[position] // shards_of).reshape([-1 if axis == position else 1 for axis in range(len(shape))])
    return loudness


def gaussian(key, extent, deviation, limit, cuts=(), dtype=jnp.bfloat16):
    array = deviation * jax.random.normal(key, extent, jnp.float32)
    if cuts:
        array = array * block_levels(key, extent, cuts, -0.22, 0.18)
    return jnp.clip(array, -limit, limit).astype(dtype)


def setup_inputs(seed: int = 0) -> dict:
    arg_keys = jax.random.split(jax.random.key(seed), 10)
    return {
        "right_sides": gaussian(arg_keys[0], (LEVELS, NRHS, FRONT), 1.0, 6.0, ((0, 4), (2, 64)), jnp.float32),
        "leaf_gen": draw_leaf_gen(jax.random.fold_in(arg_keys[9], 71), 0),
        "leaf_inverse": gaussian(arg_keys[2], (LEVELS, LEAVES * RED, RED), RED ** -0.5, 0.5, ((0, 4), (1, 64)), jnp.float32),
        "leaf_lower": gaussian(arg_keys[3], (LEVELS, LEAVES * RED, R), RED ** -0.5, 0.5, ((0, 4), (1, 64)), jnp.float32),
        "node_gen": draw_node_gen(jax.random.fold_in(arg_keys[9], 71), 0),
        "node_inverse": draw_node_inverse(jax.random.fold_in(arg_keys[9], 71), 0),
        "node_lower": draw_node_lower(jax.random.fold_in(arg_keys[9], 71), 0),
        "coupling": gaussian(arg_keys[7], (LEVELS, R, LEAF), R ** -0.5, 0.5, ((0, 4),), jnp.float32),
        "child_leaf": plant(jax.random.randint(arg_keys[8], (LEVELS,), 0, LEAVES), jax.random.fold_in(arg_keys[8], 1), 0, LEAVES - 1).astype(jnp.int32),
    }


exact_mode = lax.Precision.HIGHEST

def product(left, right):
    return jnp.matmul(left.astype(jnp.float32), right.astype(jnp.float32), precision=exact_mode)

def reference(right_sides, leaf_gen, leaf_inverse, leaf_lower, node_gen, node_inverse, node_lower, coupling, child_leaf):
    leaf_list = []
    node_list = []
    root_list = []
    incoming = jnp.zeros((NRHS, R), jnp.float32)
    for depth_index in range(LEVELS):
        update = product(incoming, coupling[depth_index])
        row_start = (child_leaf[depth_index] * LEAF).astype(jnp.int32)
        front_rhs = right_sides[depth_index]
        leaf_block = lax.dynamic_slice_in_dim(front_rhs, row_start, LEAF, 1)
        front_rhs = lax.dynamic_update_slice_in_dim(front_rhs, leaf_block + update, row_start, 1)
        pieces = front_rhs.reshape(NRHS, LEAVES, LEAF).transpose(1, 0, 2)
        turned = product(pieces, leaf_gen[depth_index].reshape(LEAVES, LEAF, LEAF))
        solved = product(turned[:, :, :RED], leaf_inverse[depth_index].reshape(LEAVES, RED, RED))
        skeleton = turned[:, :, RED:] - product(solved, leaf_lower[depth_index].reshape(LEAVES, RED, R))
        leaf_list.append(solved.transpose(1, 0, 2).reshape(NRHS, LEAVES * RED))
        per_tier = []
        for tier_index in range(HEIGHT):
            group_span = 2 ** (tier_index + 1)
            joined = jnp.concatenate([skeleton[0::2], skeleton[1::2]], axis=2)
            turned = product(joined, node_gen[depth_index, ::group_span, tier_index])
            solved = product(turned[:, :, :R], node_inverse[depth_index, ::group_span, tier_index])
            skeleton = turned[:, :, R:] - product(solved, node_lower[depth_index, ::group_span, tier_index])
            per_tier.append(jnp.repeat(solved, group_span, axis=0))
        node_list.append(jnp.stack(per_tier, axis=1))
        incoming = skeleton[0]
        root_list.append(incoming)
    return (jnp.stack(leaf_list), jnp.stack(node_list), jnp.stack(root_list))
```

```python
import jax
import jax.numpy as jnp
from jax import lax
from jax.experimental import pallas as pl
from jax.experimental.pallas import tpu as pltpu
from jax.sharding import Mesh
from jax.sharding import PartitionSpec as P

MESH = pl.DeviceIdType.MESH
BLK = ("blk_0", "blk_1", "blk_2")
BF = jnp.bfloat16
F32 = jnp.float32
NB, RHS, MAP = 16, 32, 8
ROWS = RHS + MAP


def split(value):
    high = value.astype(BF)
    return high, (value - high.astype(F32)).astype(BF)


def dot(left, right):
    return jnp.dot(left, right, preferred_element_type=F32)


def dot3(left, right):
    (lh, ll), (rh, rl) = left, right
    return dot(lh, rh) + (dot(lh, rl) + dot(ll, rh))


def kernel(
    child, x_in, lg_in, li_in, ll_in, ng_in, ni_in, nl_in, cp_in,
    leaf_out, node_out, root_out,
    xb, cp, gen, inv, low, wh, wl,
    sk0, sk1, sk2, sk3, sk4, sk5, rc0, rc1, rc2, rc3, rc4, rc5,
    ag, mr, yin, ynext, inc, mh, ml, ob,
    in_sem, up_s, up_r, z_s, z_r, m_s, m_r, i_s, i_r, d_s, d_r, y_s, y_r, out_sem,
):
    lv = lax.axis_index("level")
    x = lax.axis_index("blk_0")
    z = lax.axis_index("blk_1")
    c = lax.axis_index("blk_2")
    position = (x * 8 + z) * 2 + c
    sk = (sk0, sk1, sk2, sk3, sk4, sk5)
    rc = (rc0, rc1, rc2, rc3, rc4, rc5)

    loads = [
        pltpu.make_async_copy(src, dst, in_sem.at[k])
        for k, (src, dst) in enumerate(
            (
                (lg_in, gen.at[0]),
                (li_in, inv.at[0]),
                (ll_in, low.at[0]),
                (x_in, xb.at[:, pl.ds(0, RHS)]),
                (cp_in, cp),
                (ni_in, inv.at[pl.ds(1, 6)]),
                (nl_in, low.at[pl.ds(1, 6)]),
                (ng_in, gen.at[pl.ds(1, 6)]),
            )
        )
    ]
    for load in loads:
        load.start()

    def bit(value, k):
        return lax.rem(value // (2**k), 2)

    def flipped(value, k):
        out = value
        for j in range(3):
            if k >> j & 1:
                out = out + (1 - 2 * bit(value, j)) * 2**j
        return out

    peer_z = [flipped(z, k) for k in range(8)]
    peer_x = (flipped(x, 1), flipped(x, 2))
    core_peer = (lv, x, z, 1 - c)

    barrier = pltpu.get_barrier_semaphore()

    def greet(device):
        pl.semaphore_signal(barrier, inc=1, device_id=device, device_id_type=MESH)

    greet(core_peer)
    for k in range(1, 8):
        greet((lv, x, peer_z[k], c))
        greet((lv, x, peer_z[k], 1 - c))
    greet((lv, peer_x[0], z, c))
    greet((lv, peer_x[1], z, c))

    @pl.when(lv > 0)
    def _():
        greet((lv - 1, x, z, c))

    @pl.when(lv < 3)
    def _():
        greet((lv + 1, x, z, c))

    def fold(t):
        g_first, g_last = gen[t, :, :128], gen[t, :, 128:]
        first = dot3(split(g_first), split(inv[t]))
        last = g_last - dot3(split(first), split(low[t]))
        high, rest = split(first)
        wh[t, :, :128] = high
        wl[t, :, :128] = rest
        high, rest = split(last)
        wh[t, :, 128:] = high
        wl[t, :, 128:] = rest

    def remote(src, dst, send, recv, device):
        return pltpu.make_async_remote_copy(
            src_ref=src, dst_ref=dst, send_sem=send, recv_sem=recv, device_id=device, device_id_type=MESH
        )

    for k in (0, 1, 2):
        loads[k].wait()
    fold(0)
    loads[3].wait()
    loads[4].wait()
    is_target = child[0] == position
    xb[:, RHS:] = jnp.where(is_target, cp[...], jnp.zeros_like(cp))

    def leaf_chunk(k, carry):
        rows = xb[pl.ds(k * 4, 4)].reshape(4 * ROWS, 256)
        y = dot3(split(rows), (wh[0], wl[0]))
        ag[7, pl.ds(k * 4, 4)] = y[:, :128].reshape(4, ROWS, 128)
        sk0[pl.ds(k * 4, 4)] = y[:, 128:].reshape(4, ROWS, 128)
        return carry

    lax.fori_loop(0, 4, leaf_chunk, 0)

    pl.semaphore_wait(barrier, 17 + jnp.minimum(lv, 1) + jnp.minimum(3 - lv, 1))

    zb = [bit(z, k) for k in range(3)]
    sides = (c, zb[0], zb[1], zb[2], bit(x, 0), bit(x, 1))
    partners = (
        core_peer,
        (lv, x, peer_z[1], c),
        (lv, x, peer_z[2], c),
        (lv, x, peer_z[4], c),
        (lv, peer_x[0], z, c),
        (lv, peer_x[1], z, c),
    )
    starts = [c * 8]
    for h in range(1, 4):
        starts.append(starts[-1] + sides[h] * (8 >> h))
    q = starts[3]
    starts += [q, q]

    def send_z(g, h, blocks, ks):
        out = []
        for k in ks:
            ref = ag.at[h, blocks]
            out.append(remote(ref, ref, z_s.at[g, k], z_r.at[g, k], (lv, x, peer_z[k], c)))
        return out

    def send_core(g, tiers):
        half = ag.at[tiers, pl.ds(c * 8, 8)]
        return remote(half, half, d_s.at[g], d_r.at[g], core_peer)

    relays = [send_core(h, pl.ds(h, 1)) for h in range(4)] + [send_core(4, pl.ds(4, 3))]
    gathers = [
        send_z(0, 1, pl.ds(starts[1], 4), (1,)),
        send_z(1, 2, pl.ds(starts[2], 2), (1, 2, 3)),
        send_z(2, 3, pl.ds(q, 1), range(1, 8)),
    ]
    tops = []
    for k in range(1, 8):
        ref = ag.at[pl.ds(4, 3), pl.ds(q, 1)]
        tops.append(remote(ref, ref, z_s.at[3, k], z_r.at[3, k], (lv, x, peer_z[k], c)))

    ups = []
    for h in range(6):
        side = sides[h]
        count = 8 >> h if h < 4 else 1
        keep = side * count if h < 4 else 0
        give = (1 - side) * count if h < 4 else 0
        up = remote(sk[h].at[pl.ds(give, count)], rc[h], up_s.at[h], up_r.at[h], partners[h])
        up.start()
        ups.append(up)
        if h == 4:
            for group in gathers:
                for copy in group:
                    copy.start()
        if h == 0:
            loads[5].wait()
            loads[6].wait()
            loads[7].wait()
        fold(h + 1)
        up.wait_recv()
        mine_rows = pl.ds(pl.multiple_of(side * 128, 128), 128)
        other_rows = pl.ds(pl.multiple_of((1 - side) * 128, 128), 128)
        step = min(count, 4)
        for k in range(0, count, step):
            mine = sk[h][pl.ds(keep + k, step)].reshape(step * ROWS, 128)
            other = rc[h][pl.ds(k, step)].reshape(step * ROWS, 128)
            y = dot3(split(mine), (wh[h + 1, mine_rows], wl[h + 1, mine_rows]))
            y = y + dot3(split(other), (wh[h + 1, other_rows], wl[h + 1, other_rows]))
            ag[h, pl.ds(starts[h] + k, step)] = y[:, :128].reshape(step, ROWS, 128)
            skeleton = y[:, 128:].reshape(step, ROWS, 128)
            if h < 5:
                sk[h + 1][pl.ds(k, step)] = skeleton
            else:
                ag[6, pl.ds(q, 1)] = skeleton
                mr[pl.ds(q, 1)] = skeleton[:, RHS:]
                ynext[...] = skeleton[:, :RHS]
        if h == 0:
            relays[0].start()

    maps = []
    for k in range(8):
        for side in range(2):
            if k or side:
                ref = mr.at[pl.ds(q, 1)]
                device = (lv, x, peer_z[k], 1 - c if side else c)
                maps.append(remote(ref, ref, m_s.at[2 * k + side], m_r.at[2 * k + side], device))
    for copy in maps:
        copy.start()
    chain = remote(ynext, yin, y_s, y_r, (lv + 1, x, z, c))
    incs = []
    for k in range(1, 8):
        ref = inc.at[pl.ds(q, 1)]
        incs.append(remote(ref, ref, i_s.at[k], i_r.at[k], (lv, x, peer_z[k], c)))
    half = inc.at[pl.ds(c * 8, 8)]
    inc_relay = remote(half, half, d_s.at[5], d_r.at[5], core_peer)

    @pl.when(lv == 0)
    def _():
        chain.start()

    for copy in tops:
        copy.start()
    for g in range(3):
        for copy in gathers[g]:
            copy.wait_recv()
        relays[g + 1].start()
    for copy in maps:
        copy.wait_recv()

    @pl.when(lv == 0)
    def _():
        inc[...] = jnp.zeros_like(inc)

    @pl.when(lv > 0)
    def _():
        chain.wait_recv()
        inc[pl.ds(q, 1)] = yin[...]
        for copy in incs:
            copy.start()

    @pl.when((lv > 0) & (lv < 3))
    def _():
        root_map = mr[...].reshape(128, 128)
        ynext[...] = ynext[...] + dot3(split(yin[...].reshape(RHS, 128)), split(root_map)).reshape(1, RHS, 128)
        chain.start()

    for copy in tops:
        copy.wait_recv()
    relays[4].start()
    for relay in relays:
        relay.wait_recv()

    def split_maps(t, carry):
        high, rest = split(ag[t, :, RHS:].reshape(128, 128))
        mh[t] = high
        ml[t] = rest
        return carry

    lax.fori_loop(0, 8, split_maps, 0)

    @pl.when(lv > 0)
    def _():
        for copy in incs:
            copy.wait_recv()
        inc_relay.start()
        inc_relay.wait_recv()

    def correct(t, carry):
        for k in range(0, NB, 8):
            rows = inc[pl.ds(k, 8)].reshape(8 * RHS, 128)
            update = dot3(split(rows), (mh[t], ml[t]))
            ob[t, pl.ds(k, 8)] = ag[t, pl.ds(k, 8), :RHS] + update.reshape(8, RHS, 128)
        return carry

    lax.fori_loop(0, 8, correct, 0)
    stores = [
        pltpu.make_async_copy(ob.at[pl.ds(0, 6)], node_out, out_sem.at[0]),
        pltpu.make_async_copy(ob.at[6], root_out, out_sem.at[1]),
        pltpu.make_async_copy(ob.at[7], leaf_out, out_sem.at[2]),
    ]
    for store in stores:
        store.start()

    for copy in ups + tops + maps + relays + [copy for group in gathers for copy in group]:
        copy.wait_send()

    @pl.when(lv > 0)
    def _():
        for copy in incs + [inc_relay]:
            copy.wait_send()

    @pl.when(lv < 3)
    def _():
        chain.wait_send()

    for store in stores:
        store.wait()


def shards(
    right_sides, leaf_gen, leaf_inverse, leaf_lower, node_gen, node_inverse, node_lower, coupling, child_leaf
):
    any_space = pl.BlockSpec(memory_space=pl.ANY)
    dma = pltpu.SemaphoreType.DMA
    vm = pltpu.VMEM
    counts = (16, 8, 4, 2, 1, 1)
    leaf, node, root = pl.pallas_call(
        kernel,
        out_shape=(
            jax.ShapeDtypeStruct((NB, RHS, 128), F32),
            jax.ShapeDtypeStruct((6, NB, RHS, 128), F32),
            jax.ShapeDtypeStruct((NB, RHS, 128), F32),
        ),
        in_specs=[pl.BlockSpec(memory_space=pltpu.SMEM)] + [any_space] * 8,
        out_specs=(any_space,) * 3,
        scratch_shapes=[
            vm((NB, ROWS, 256), F32),
            vm((NB, MAP, 256), F32),
            vm((7, 256, 256), F32),
            vm((7, 128, 128), F32),
            vm((7, 128, 128), F32),
            vm((7, 256, 256), BF),
            vm((7, 256, 256), BF),
        ]
        + [vm((n, ROWS, 128), F32) for n in counts]
        + [vm((n, ROWS, 128), F32) for n in (8, 4, 2, 1, 1, 1)]
        + [
            vm((8, NB, ROWS, 128), F32),
            vm((NB, MAP, 128), F32),
            vm((1, RHS, 128), F32),
            vm((1, RHS, 128), F32),
            vm((NB, RHS, 128), F32),
            vm((8, 128, 128), BF),
            vm((8, 128, 128), BF),
            vm((8, NB, RHS, 128), F32),
            dma((8,)),
            dma((6,)),
            dma((6,)),
            dma((4, 8)),
            dma((4, 8)),
            dma((16,)),
            dma((16,)),
            dma((8,)),
            dma((8,)),
            dma((6,)),
            dma((6,)),
            dma,
            dma,
            dma((3,)),
        ],
        compiler_params=pltpu.CompilerParams(
            collective_id=0, has_side_effects=True, vmem_limit_bytes=40 * 1024 * 1024
        ),
    )(
        child_leaf,
        right_sides.reshape(NB, RHS, 256),
        leaf_gen[0],
        leaf_inverse[0],
        leaf_lower[0],
        node_gen[0, 0],
        node_inverse[0, 0],
        node_lower[0, 0],
        coupling.reshape(NB, MAP, 256),
    )
    return (leaf.reshape(1, 512, 128), node.reshape(1, 1, 6, 512, 128), root.reshape(1, 512, 128))


def solution(mesh):
    split_mesh = Mesh(
        mesh.devices.reshape(mesh.shape["level"], 4, 8, 2), ("level", "blk_0", "blk_1", "blk_2")
    )
    return jax.shard_map(
        shards,
        mesh=split_mesh,
        in_specs=(
            P("level", None, BLK),
            P("level", BLK, None),
            P("level", BLK, None),
            P("level", BLK, None),
            P("level", BLK, None, None, None),
            P("level", BLK, None, None, None),
            P("level", BLK, None, None, None),
            P("level", None, None),
            P("level"),
        ),
        out_specs=(
            P("level", None, BLK),
            P("level", BLK, None, None, None),
            P("level", None, None),
        ),
        check_vma=False,
    )
```
